32 devices in a mesh: dp: 4 (over y, x), row: 2 (over core), col: 4 (over z).
Axes of the slice: x: 2, y: 2, z: 4, core: 2. Of those that a mesh axis runs over, the one named last changes fastest.
Arguments:
- tokens: bfloat16 [3840, 4096], P(('dp', 'col'), 'row'), may hold values from -6 to 6
- hidden_cot: bfloat16 [3840, 14336], P(('dp', 'row'), 'col'), may hold values from -0.09667969 to 0.09667969
- gate_pre: bfloat16 [3840, 14336], P(('dp', 'row'), 'col'), may hold values from -10 to 10
- up_pre: bfloat16 [3840, 14336], P(('dp', 'row'), 'col'), may hold values from -6 to 6
Outputs:
- grad_gate: bfloat16 [2, 2048, 14336], P('row', 'dp', 'col')
The draws below stay inside these ranges and needn't reach their ends.
All inputs are finite; a program needn't handle non-finite values.
Results may differ from the reference program's by a relative error of at most 0.014.
Values may be sent and summed in bfloat16 or wider, within the bound.
A program may use at most 128 MiB of HBM per device.

```python
import jax
import jax.numpy as jnp
from jax import lax

D = 4096
FF = 14336
GROUP_TOK = 960
TOKENS = 3840
N_DP = 4
N_ROW = 2


def level_of(own_key, shape, split, least, high):
    def one(dim, parts):
        heights = jax.random.uniform(jax.random.fold_in(jax.random.fold_in(own_key, 6), dim), (parts,), jnp.float32, least / len(split), high / len(split))
        return jnp.repeat(jnp.exp(heights), shape[dim] // parts).reshape((-1,) + (1,) * (len(shape) - dim - 1))

    gain = one(*split[0])
    for cut in split[1:]:
        gain = gain * one(*cut)
    return gain


def scatter_about(own_key, dims, deviation, most, shards=(), held_as=jnp.bfloat16):
    drawn = deviation * jax.random.normal(own_key, dims, jnp.float32)
    if shards:
        drawn = drawn * level_of(own_key, dims, shards, -0.22, 0.18)
    return jnp.clip(drawn, -most, most).astype(held_as)


def setup_inputs(seed: int = 0) -> dict:
    seeds = jax.random.split(jax.random.key(seed), 5)
    return {
        "tokens": scatter_about(seeds[0], (TOKENS, D), 1.0, 6.0, ((0, 16), (1, 2))),
        "hidden_cot": scatter_about(seeds[1], (TOKENS, FF), (TOKENS ** -0.5), 0.09667969, ((0, 8), (1, 4))),
        "gate_pre": scatter_about(seeds[2], (TOKENS, FF), 2.0, 10.0, ((0, 8), (1, 4))),
        "up_pre": scatter_about(seeds[3], (TOKENS, FF), 1.0, 6.0, ((0, 8), (1, 4))),
    }


def reference(tokens, hidden_cot, gate_pre, up_pre):
    gate_val = gate_pre.astype(jnp.float32)
    up_val = up_pre.astype(jnp.float32)
    cot_val = hidden_cot.astype(jnp.float32)
    sigma = jax.nn.sigmoid(gate_val)
    gate_grad = (cot_val * up_val * sigma * (1.0 + gate_val * (1.0 - sigma))).astype(jnp.bfloat16)
    tok_groups = tokens.reshape(N_DP, GROUP_TOK, D)
    grad_groups = gate_grad.reshape(N_DP, GROUP_TOK, FF)

    def one_group(total, pair):
        part = jnp.dot(pair[0].T, pair[1], preferred_element_type=jnp.float32).astype(jnp.bfloat16)
        return total + part.astype(jnp.float32), None

    summed, _ = lax.scan(one_group, jnp.zeros((D, FF), jnp.float32), (tok_groups, grad_groups))
    return summed.astype(jnp.bfloat16).reshape(N_ROW, D // N_ROW, FF)
```

```python
import functools
import math

import jax
import jax.numpy as jnp
from jax import lax
from jax.experimental import pallas as pl
from jax.experimental.pallas import tpu as pltpu
from jax.sharding import PartitionSpec as P

MESH = pl.DeviceIdType.MESH


def near_square(n):
    nx = math.isqrt(n)
    while n % nx:
        nx -= 1
    return n // nx, nx


def kernel(dims, plan, tok, cot, gate, up, out, ins, grads, toks, tokt, part, got,
           in_sem, own_sem, ty_s, ty_r, tz_s, tz_r, gy_s, gy_r, gp_s, gp_r, x_s, x_r):
    ny, nx, nr, nz, wide, block, chunks, cols = dims
    lead, ahead, own_at, per = plan
    dp, r, z = lax.axis_index("dp"), lax.axis_index("row"), lax.axis_index("col")
    y, x = dp // nx, dp % nx
    subs = wide // block
    away = (nx - 1) * subs
    blocks = nx * subs
    rows = ny * nr * grads.shape[3]

    def at(oy=0, ox=0, orow=0, oz=0):
        return {
            "dp": (y + oy) % ny * nx + (x + ox) % nx,
            "row": (r + orow) % nr,
            "col": (z + oz) % nz,
        }

    def remote(src, dst, ss, rs, to):
        return pltpu.make_async_remote_copy(
            src_ref=src, dst_ref=dst, send_sem=ss, recv_sem=rs, device_id=to, device_id_type=MESH)

    def span(low, high, f):
        def body(i, c):
            f(i)
            return c
        lax.fori_loop(low, high, body, 0)

    def load(k, i):
        src = (cot, gate, up)[i]
        return pltpu.make_async_copy(
            src.at[:, pl.ds(pl.multiple_of(k * cols, cols), cols)],
            ins.at[k, :, pl.ds(i * cols, cols)], in_sem.at[k])

    def loaded(k):
        pltpu.make_async_copy(cot.at[:, pl.ds(0, 3 * cols)], ins.at[k], in_sem.at[k]).wait()

    def tok_cols(oy, b):
        o, sub = (b // subs + 1) % nx, b % subs
        first = ((y + oy) % ny * nx + (x + o) % nx) * wide + sub * block
        return tok.at[:, pl.ds(pl.multiple_of(first, block), block)]

    def own_tok(b):
        return pltpu.make_async_copy(tok_cols(0, b), toks.at[b, y, z], own_sem.at[b])

    def tok_y(oy, b):
        return remote(tok_cols(oy, b), toks.at[b, y, z], ty_s.at[oy - 1], ty_r.at[oy - 1, b], at(oy=oy))

    reach = min(2, nz - 1)
    hops = ([(d, 0) for d in range(reach, 0, -1)] + [(1, d) for d in range(2, nz - 1)])
    relays = max(nz - 3, 0)

    def valid(way, far, back):
        left = z >= back if way > 0 else z + back < nz
        right = z + far < nz if way > 0 else z >= far
        return jnp.logical_and(left, right)

    def relay_sem(w, back, b, oy):
        return blocks + ((w * relays + back - 2) * blocks + b) * ny + oy

    def tok_z(b, oy, way, i):
        far, back = hops[i]
        ref = toks.at[b, (y - oy + ny) % ny, z - way * back]
        w, dist = (0 if way > 0 else 1), far + back
        sem = b
        if 2 <= dist <= nz - 2:
            beyond = z + way * (far + 1)
            goes_on = beyond < nz if way > 0 else beyond >= 0
            sem = jnp.where(goes_on, relay_sem(w, dist, b, oy), b)
        return remote(ref, ref, tz_s.at[w], tz_r.at[sem], at(oz=way * far + nz))

    def each_hop(relay, act):
        for i, (far, back) in enumerate(hops):
            if (back > 0) == relay:
                for way in (1, -1):
                    pl.when(valid(way, far, back))(functools.partial(act, way, i))

    def send_z(b, oy):
        each_hop(False, lambda way, i: tok_z(b, oy, way, i).start())

    def relay_z(b):
        for oy in range(ny):
            def go(way, i, oy=oy):
                back = hops[i][1]
                ref = toks.at[b, (y - oy + ny) % ny, z - way * back]
                w = 0 if way > 0 else 1
                remote(ref, ref, tz_s.at[w], tz_r.at[relay_sem(w, back, b, oy)], at(oz=1)).wait_recv()
                tok_z(b, oy, way, i).start()
            each_hop(True, go)

    def all_z(b):
        count = nz - 1
        for way in (1, -1):
            for far, back in hops:
                if back:
                    count = count - valid(way, far, back).astype(jnp.int32)
        for n in range(1, nz):
            ref = toks.at[b, :, pl.ds(0, n)]
            pl.when(count == n)(remote(ref, ref, tz_s.at[0], tz_r.at[b], at(oz=1)).wait_recv)

    def sent_z():
        for way in (1, -1):
            w = 0 if way > 0 else 1
            count = jnp.int32(0)
            for far, back in hops:
                count = count + valid(way, far, back).astype(jnp.int32)
            for n in range(1, nz):
                ref = toks.at[:, :, pl.ds(0, n)]
                pl.when(count == n)(remote(ref, ref, tz_s.at[w], tz_r.at[0], at(oz=1)).wait_send)

    def grad_y(oy, k):
        ref = grads.at[k, y, r]
        return remote(ref, ref, gy_s.at[oy - 1], gy_r.at[oy - 1, k], at(oy=oy))

    def grad_p(orow, oy, k):
        ref = grads.at[k, (y - oy + ny) % ny, r]
        return remote(ref, ref, gp_s.at[orow - 1], gp_r.at[orow - 1, k], at(orow=orow))

    def got_p(orow, k):
        ref = grads.at[k, :, (r - orow + nr) % nr]
        remote(ref, ref, gp_s.at[orow - 1], gp_r.at[orow - 1, k], at(orow=orow)).wait_recv()

    def sum_x(b, k):
        at_rows = pl.ds(pl.multiple_of(b * block, block), block)
        return remote(part.at[k, at_rows], got.at[k, at_rows], x_s.at[0], x_r.at[k], at(ox=b // subs + 1))

    span(0, blocks, lambda b: own_tok(b).start())

    def load_all(k):
        for i in range(3):
            load(k, i).start()
    span(0, chunks, load_all)

    peers = ([at(oy=o) for o in range(1, ny)] + [at(ox=o) for o in range(1, nx)]
             + [at(orow=o) for o in range(1, nr)] + [at(oz=o) for o in range(1, nz)])
    barrier = pltpu.get_barrier_semaphore()
    for to in peers:
        pl.semaphore_signal(barrier, inc=1, device_id=to, device_id_type=MESH)
    pl.semaphore_wait(barrier, len(peers))

    def tok_out(b):
        for oy in range(1, ny):
            tok_y(oy, b).start()

    def own_out(b):
        own_tok(b).wait()
        send_z(b, 0)

    def pass_on(b):
        for oy in range(1, ny):
            tok_y(oy, b).wait_recv()
            send_z(b, oy)

    def gate_grad(k):
        loaded(k)
        step = 32
        tall = ins.shape[1]

        def rows_of(j, c):
            at_rows = pl.ds(pl.multiple_of(j * step, step), step)
            h = ins[k, at_rows, 0:cols].astype(jnp.float32)
            g = ins[k, at_rows, cols:2 * cols].astype(jnp.float32)
            u = ins[k, at_rows, 2 * cols:3 * cols].astype(jnp.float32)
            s = jax.nn.sigmoid(g)
            grads[k, y, r, at_rows, :] = (h * u * s * (1.0 + g * (1.0 - s))).astype(grads.dtype)
            return c
        lax.fori_loop(0, tall // step, rows_of, 0)
        for oy in range(1, ny):
            grad_y(oy, k).start()
        for orow in range(1, nr):
            grad_p(orow, 0, k).start()

    def feed(k):
        gate_grad(k)
        pl.when(k + 1 < blocks)(lambda: tok_out(k + 1))

    def take_block(b):
        all_z(b)
        first = pl.multiple_of(b * block, block)
        tokt[pl.ds(first, block), :] = toks[b].reshape(rows, block).T

    def tile(b, k):
        at_rows = pl.ds(pl.multiple_of(b * block, block), block)
        right = grads[k].reshape(rows, cols)
        sums = jnp.dot(tokt[at_rows, :], right, preferred_element_type=jnp.float32)
        part[k, at_rows, :] = sums.astype(part.dtype)
        sum_x(b, k).start()

    def finish(k):
        left = tokt[away * block:, :]
        sums = jnp.dot(left, grads[k].reshape(rows, cols), preferred_element_type=jnp.float32)
        remote(got.at[k], got.at[k], x_s.at[0], x_r.at[k], at(ox=1)).wait_recv()
        for o in range(nx - 1):
            sums = sums + got[k, o * wide:(o + 1) * wide, :].astype(jnp.float32)
        out[0, :, pl.ds(pl.multiple_of(k * cols, cols), cols)] = sums.astype(out.dtype)

    def catch_up(k, b):
        take_block(b)
        span(0, k, functools.partial(tile, b))

    def pass_step(j):
        pass_on(j)
        pl.when(j + 1 < blocks)(lambda: own_out(j + 1))

    passed = lambda k: jnp.minimum(k + 2, blocks)
    relayed = lambda k: jnp.clip(jnp.where(k < away, k + 1, away + (k - away) * 5 // 6), 0, blocks)
    ready = lambda k: jnp.clip(k, 1, away)
    ended = lambda k: jnp.clip((k - own_at + 1) * per, 0, jnp.maximum(k - 1, 0))

    tok_out(0)
    own_out(0)
    span(0, lead, feed)
    pass_step(0)
    span(lead, ahead, feed)

    def main(k, c):
        span(jnp.where(k > 0, ready(k - 1), 1), ready(k), functools.partial(catch_up, k))
        for oy in range(1, ny):
            grad_y(oy, k).wait_recv()
            for orow in range(1, nr):
                grad_p(orow, oy, k).start()
        span(jnp.where(k > 0, relayed(k - 1), 0), relayed(k), relay_z)
        span(passed(k - 1), passed(k), pass_step)
        pl.when(k + ahead < chunks)(lambda: feed(k + ahead))
        pl.when(k == 0)(lambda: take_block(0))
        for orow in range(1, nr):
            got_p(orow, k)
        span(0, ready(k), lambda b: tile(b, k))

        @pl.when(k == own_at)
        def _():
            span(away, blocks, take_block)
        span(ended(k - 1), ended(k), finish)
        return c
    lax.fori_loop(0, chunks, main, 0)
    span(ended(chunks - 1), chunks, finish)

    for oy in range(1, ny):
        ref = toks.at[:, y, z]
        remote(ref, ref, ty_s.at[oy - 1], ty_r.at[oy - 1, 0], at(oy=oy)).wait_send()
        ref = grads.at[:, y, r]
        remote(ref, ref, gy_s.at[oy - 1], gy_r.at[oy - 1, 0], at(oy=oy)).wait_send()
    for orow in range(1, nr):
        ref = grads.at[:, :, r]
        remote(ref, ref, gp_s.at[orow - 1], gp_r.at[orow - 1, 0], at(orow=orow)).wait_send()
    sent_z()
    remote(part, part, x_s.at[0], x_r.at[0], at(ox=1)).wait_send()


def solution(mesh):
    ndp, nr, nz = mesh.shape["dp"], mesh.shape["row"], mesh.shape["col"]
    ny, nx = near_square(ndp)

    def on_device(tokens, hidden_cot, gate_pre, up_pre):
        tok_rows, wid = tokens.shape
        tall, hidden = gate_pre.shape
        wide = wid // ndp
        block = math.gcd(wide, 128)
        cols = math.gcd(hidden, 256)
        chunks = hidden // cols
        subs = wide // block
        blocks, away = nx * subs, (nx - 1) * subs
        rows = ny * nz * tok_rows
        relays = 2 * max(nz - 3, 0) * blocks * ny
        dims = (ny, nx, nr, nz, wide, block, chunks, cols)
        plan = (3, min(5, chunks), max(chunks - 4, 0), 4)
        dma = pltpu.SemaphoreType.DMA
        dt = tokens.dtype
        return pl.pallas_call(
            functools.partial(kernel, dims, plan),
            out_shape=pltpu.VMEM((1, wide, hidden), dt),
            in_specs=[pl.BlockSpec(memory_space=pl.ANY)] * 4,
            out_specs=pl.BlockSpec(memory_space=pltpu.VMEM),
            scratch_shapes=[
                pltpu.VMEM((chunks, tall, 3 * cols), dt),
                pltpu.VMEM((chunks, ny, nr, tall, cols), dt),
                pltpu.VMEM((blocks, ny, nz, tok_rows, block), dt),
                pltpu.VMEM((blocks * block, rows), dt),
                pltpu.VMEM((chunks, away * block, cols), dt),
                pltpu.VMEM((chunks, away * block, cols), dt),
                dma((chunks,)),
                dma((blocks,)),
                dma((ny - 1,)),
                dma((ny - 1, blocks)),
                dma((2,)),
                dma((blocks + relays,)),
                dma((ny - 1,)),
                dma((ny - 1, chunks)),
                dma((nr - 1,)),
                dma((nr - 1, chunks)),
                dma((1,)),
                dma((chunks,)),
            ],
            compiler_params=pltpu.CompilerParams(
                collective_id=0, has_side_effects=True, vmem_limit_bytes=56 * 1024 * 1024
            ),
        )(tokens, hidden_cot, gate_pre, up_pre)

    in_specs = (
        P(("dp", "col"), "row"),
        P(("dp", "row"), "col"),
        P(("dp", "row"), "col"),
        P(("dp", "row"), "col"),
    )
    return jax.shard_map(
        on_device, mesh=mesh, in_specs=in_specs, out_specs=P("row", "dp", "col"), check_vma=False
    )
```

```python
import functools
import math

import jax
import jax.numpy as jnp
from jax import lax
from jax.experimental import pallas as pl
from jax.experimental.pallas import tpu as pltpu
from jax.sharding import PartitionSpec as P

MESH = pl.DeviceIdType.MESH


def near_square(n):
    nx = math.isqrt(n)
    while n % nx:
        nx -= 1
    return n // nx, nx


def kernel(dims, plan, tok, cot, gate, up, out, ins, grads, toks, tokt, part, got,
           in_sem, own_sem, ty_s, ty_r, tz_s, tz_r, gy_s, gy_r, gp_s, gp_r, x_s, x_r):
    ny, nx, nr, nz, wide, block, chunks, cols = dims
    lead, ahead, own_at, per = plan
    dp, r, z = lax.axis_index("dp"), lax.axis_index("row"), lax.axis_index("col")
    y, x = dp // nx, dp % nx
    subs = wide // block
    away = (nx - 1) * subs
    blocks = nx * subs
    rows = ny * nr * grads.shape[3]

    def at(oy=0, ox=0, orow=0, oz=0):
        return {
            "dp": (y + oy) % ny * nx + (x + ox) % nx,
            "row": (r + orow) % nr,
            "col": (z + oz) % nz,
        }

    def remote(src, dst, ss, rs, to):
        return pltpu.make_async_remote_copy(
            src_ref=src, dst_ref=dst, send_sem=ss, recv_sem=rs, device_id=to, device_id_type=MESH)

    def span(low, high, f):
        def body(i, c):
            f(i)
            return c
        lax.fori_loop(low, high, body, 0)

    def load(k, i):
        at_cols = pl.ds(0, cols) if k == 0 else pl.ds(cols, (chunks - 1) * cols)
        return pltpu.make_async_copy((cot, gate, up)[i].at[:, at_cols], ins.at[i, :, at_cols], in_sem.at[i, k])

    def loads(k, act):
        for i in range(3):
            act(load(k, i))

    def tok_cols(oy, b):
        o, sub = (b // subs + 1) % nx, b % subs
        first = ((y + oy) % ny * nx + (x + o) % nx) * wide + sub * block
        return tok.at[:, pl.ds(pl.multiple_of(first, block), block)]

    def own_tok(b):
        return pltpu.make_async_copy(tok_cols(0, b), toks.at[b, y, z], own_sem.at[b])

    def tok_y(oy, b):
        return remote(tok_cols(oy, b), toks.at[b, y, z], ty_s.at[oy - 1], ty_r.at[oy - 1, b], at(oy=oy))

    reach = min(2, nz - 1)
    hops = ([(d, 0) for d in range(reach, 0, -1)] + [(1, d) for d in range(2, nz - 1)])
    relays = max(nz - 3, 0)

    def valid(way, far, back):
        left = z >= back if way > 0 else z + back < nz
        right = z + far < nz if way > 0 else z >= far
        return jnp.logical_and(left, right)

    def relay_sem(w, back, b, oy):
        w = w if nz > 4 else 0
        return blocks + ((w * relays + back - 2) * blocks + b) * ny + oy

    def goes_on(way, far, back):
        if not 2 <= far + back <= nz - 2:
            return jnp.bool_(False)
        beyond = z + way * (far + 1)
        return beyond < nz if way > 0 else beyond >= 0

    def tok_z(b, oy, way, i):
        far, back = hops[i]
        ref = toks.at[b, (y - oy + ny) % ny, z - way * back]
        w, dist = (0 if way > 0 else 1), far + back
        sem = jnp.where(goes_on(way, far, back), relay_sem(w, dist, b, oy), b)
        return remote(ref, ref, tz_s.at[w], tz_r.at[sem], at(oz=way * far + nz))

    def each_hop(relay, act):
        for i, (far, back) in enumerate(hops):
            if (back > 0) == relay:
                for way in (1, -1):
                    pl.when(valid(way, far, back))(functools.partial(act, way, i))

    def send_z(b, oy, part):
        def go(way, i):
            far, back = hops[i]
            send = tok_z(b, oy, way, i).start
            if part == "all":
                send()
            elif part == "far":
                pl.when(goes_on(way, far, back))(send)
            else:
                pl.when(jnp.logical_not(goes_on(way, far, back)))(send)
        each_hop(False, go)

    def relay_z(group, b):
        for oy in group:
            def go(way, i, oy=oy):
                back = hops[i][1]
                ref = toks.at[b, (y - oy + ny) % ny, z - way * back]
                w = 0 if way > 0 else 1
                remote(ref, ref, tz_s.at[w], tz_r.at[relay_sem(w, back, b, oy)], at(oz=1)).wait_recv()
                tok_z(b, oy, way, i).start()
            each_hop(True, go)

    def all_z(b):
        count = nz - 1
        for way in (1, -1):
            for far, back in hops:
                if back:
                    count = count - valid(way, far, back).astype(jnp.int32)
        for n in range(1, nz):
            ref = toks.at[b, :, pl.ds(0, n)]
            pl.when(count == n)(remote(ref, ref, tz_s.at[0], tz_r.at[b], at(oz=1)).wait_recv)

    def sent_z():
        for way in (1, -1):
            w = 0 if way > 0 else 1
            count = jnp.int32(0)
            for far, back in hops:
                count = count + valid(way, far, back).astype(jnp.int32)
            for n in range(1, nz):
                ref = toks.at[:, :, pl.ds(0, n)]
                pl.when(count == n)(remote(ref, ref, tz_s.at[w], tz_r.at[0], at(oz=1)).wait_send)

    def grad_y(oy, k):
        ref = grads.at[k, y, r]
        return remote(ref, ref, gy_s.at[oy - 1], gy_r.at[oy - 1, k], at(oy=oy))

    def grad_p(orow, oy, k):
        ref = grads.at[k, (y - oy + ny) % ny, r]
        return remote(ref, ref, gp_s.at[orow - 1], gp_r.at[orow - 1, k], at(orow=orow))

    def got_p(orow, k):
        ref = grads.at[k, :, (r - orow + nr) % nr]
        remote(ref, ref, gp_s.at[orow - 1], gp_r.at[orow - 1, k], at(orow=orow)).wait_recv()

    def sum_x(b, k):
        at_rows = pl.ds(pl.multiple_of(b * block, block), block)
        return remote(part.at[k, at_rows], got.at[k, at_rows], x_s.at[0], x_r.at[k], at(ox=b // subs + 1))

    span(0, blocks, lambda b: own_tok(b).start())

    for k in range(2):
        loads(k, lambda c: c.start())

    peers = ([at(oy=o) for o in range(1, ny)] + [at(ox=o) for o in range(1, nx)]
             + [at(orow=o) for o in range(1, nr)] + [at(oz=o) for o in range(1, nz)])
    barrier = pltpu.get_barrier_semaphore()
    for to in peers:
        pl.semaphore_signal(barrier, inc=1, device_id=to, device_id_type=MESH)
    pl.semaphore_wait(barrier, len(peers))

    def tok_out(b):
        for oy in range(1, ny):
            tok_y(oy, b).start()

    def own_out(b):
        own_tok(b).wait()
        send_z(b, 0, "far")

    def pass_on(b):
        for oy in range(1, ny):
            tok_y(oy, b).wait_recv()
            send_z(b, oy, "all")

    def gate_grad(k):
        for g in range(2):
            pl.when(k == g)(functools.partial(loads, g, lambda c: c.wait()))
        step = 32
        tall = ins.shape[1]
        at_cols = pl.ds(pl.multiple_of(k * cols, cols), cols)

        def rows_of(j, c):
            at_rows = pl.ds(pl.multiple_of(j * step, step), step)
            h = ins[0, at_rows, at_cols].astype(jnp.float32)
            g = ins[1, at_rows, at_cols].astype(jnp.float32)
            u = ins[2, at_rows, at_cols].astype(jnp.float32)
            s = jax.nn.sigmoid(g)
            grads[k, y, r, at_rows, :] = (h * u * s * (1.0 + g * (1.0 - s))).astype(grads.dtype)
            return c
        lax.fori_loop(0, tall // step, rows_of, 0)
        for oy in range(1, ny):
            grad_y(oy, k).start()
        for orow in range(1, nr):
            grad_p(orow, 0, k).start()

    def feed(k):
        gate_grad(k)
        pl.when(k + 1 < blocks)(lambda: tok_out(k + 1))

    def take_block(b):
        all_z(b)
        first = pl.multiple_of(b * block, block)
        tokt[pl.ds(first, block), :] = toks[b].reshape(rows, block).T

    def tile(b, k):
        at_rows = pl.ds(pl.multiple_of(b * block, block), block)
        right = grads[k].reshape(rows, cols)
        sums = jnp.dot(tokt[at_rows, :], right, preferred_element_type=jnp.float32)
        part[k, at_rows, :] = sums.astype(part.dtype)
        sum_x(b, k).start()

    def finish(k):
        left = tokt[away * block:, :]
        sums = jnp.dot(left, grads[k].reshape(rows, cols), preferred_element_type=jnp.float32)
        remote(got.at[k], got.at[k], x_s.at[0], x_r.at[k], at(ox=1)).wait_recv()
        for o in range(nx - 1):
            sums = sums + got[k, o * wide:(o + 1) * wide, :].astype(jnp.float32)
        out[0, :, pl.ds(pl.multiple_of(k * cols, cols), cols)] = sums.astype(out.dtype)

    def catch_up(k, b):
        take_block(b)
        span(0, k, functools.partial(tile, b))

    def pass_step(j):
        pass_on(j)
        pl.when(j + 1 < blocks)(lambda: own_out(j + 1))

    passed = lambda k: jnp.minimum(k + 2, blocks)
    rest = lambda b: send_z(b, 0, "rest")
    own_relay = functools.partial(relay_z, (0,))
    got_relay = functools.partial(relay_z, range(1, ny))
    early = lambda k: jnp.minimum(relayed(k) + 1, blocks)
    relayed = lambda k: jnp.clip(jnp.where(k < away, k + 1, away + (k - away) * 5 // 6), 0, blocks)
    ready = lambda k: jnp.clip(k, 1, away)
    ended = lambda k: jnp.clip((k - own_at + 1) * per, 0, jnp.maximum(k - 1, 0))

    tok_out(0)
    own_out(0)
    rest(0)
    span(0, lead, feed)
    pass_step(0)
    span(lead, ahead, feed)
    own_relay(0)

    def main(k, c):
        late = k == away
        span(jnp.where(late, away, ready(k - 1)), ready(k), functools.partial(catch_up, k))
        for oy in range(1, ny):
            grad_y(oy, k).wait_recv()
            for orow in range(1, nr):
                grad_p(orow, oy, k).start()
        before = jnp.where(k > 0, relayed(k - 1), 0)
        span(before, relayed(k), got_relay)
        span(jnp.where(late, ready(k - 1), away), away, functools.partial(catch_up, k))
        span(passed(k - 1), passed(k), rest)
        span(jnp.minimum(before + 1, blocks), early(k), own_relay)
        span(passed(k - 1), passed(k), pass_step)
        pl.when(k + ahead < chunks)(lambda: feed(k + ahead))
        pl.when(k == 0)(lambda: take_block(0))
        for orow in range(1, nr):
            got_p(orow, k)
        span(0, ready(k), lambda b: tile(b, k))

        @pl.when(k == own_at)
        def _():
            span(away, blocks, take_block)
        span(ended(k - 1), ended(k), finish)
        return c
    lax.fori_loop(0, chunks, main, 0)
    span(ended(chunks - 1), chunks, finish)

    for oy in range(1, ny):
        ref = toks.at[:, y, z]
        remote(ref, ref, ty_s.at[oy - 1], ty_r.at[oy - 1, 0], at(oy=oy)).wait_send()
        ref = grads.at[:, y, r]
        remote(ref, ref, gy_s.at[oy - 1], gy_r.at[oy - 1, 0], at(oy=oy)).wait_send()
    for orow in range(1, nr):
        ref = grads.at[:, :, r]
        remote(ref, ref, gp_s.at[orow - 1], gp_r.at[orow - 1, 0], at(orow=orow)).wait_send()
    sent_z()
    remote(part, part, x_s.at[0], x_r.at[0], at(ox=1)).wait_send()


def solution(mesh):
    ndp, nr, nz = mesh.shape["dp"], mesh.shape["row"], mesh.shape["col"]
    ny, nx = near_square(ndp)

    def on_device(tokens, hidden_cot, gate_pre, up_pre):
        tok_rows, wid = tokens.shape
        tall, hidden = gate_pre.shape
        wide = wid // ndp
        block = math.gcd(wide, 128)
        cols = math.gcd(hidden, 256)
        chunks = hidden // cols
        subs = wide // block
        blocks, away = nx * subs, (nx - 1) * subs
        rows = ny * nz * tok_rows
        relays = (2 if nz > 4 else 1) * max(nz - 3, 0) * blocks * ny
        dims = (ny, nx, nr, nz, wide, block, chunks, cols)
        plan = (3, min(5, chunks), max(chunks - 4, 0), 4)
        dma = pltpu.SemaphoreType.DMA
        dt = tokens.dtype
        return pl.pallas_call(
            functools.partial(kernel, dims, plan),
            out_shape=pltpu.VMEM((1, wide, hidden), dt),
            in_specs=[pl.BlockSpec(memory_space=pl.ANY)] * 4,
            out_specs=pl.BlockSpec(memory_space=pltpu.VMEM),
            scratch_shapes=[
                pltpu.VMEM((3, tall, hidden), dt),
                pltpu.VMEM((chunks, ny, nr, tall, cols), dt),
                pltpu.VMEM((blocks, ny, nz, tok_rows, block), dt),
                pltpu.VMEM((blocks * block, rows), dt),
                pltpu.VMEM((chunks, away * block, cols), dt),
                pltpu.VMEM((chunks, away * block, cols), dt),
                dma((3, 2)),
                dma((blocks,)),
                dma((ny - 1,)),
                dma((ny - 1, blocks)),
                dma((2,)),
                dma((blocks + relays,)),
                dma((ny - 1,)),
                dma((ny - 1, chunks)),
                dma((nr - 1,)),
                dma((nr - 1, chunks)),
                dma((1,)),
                dma((chunks,)),
            ],
            compiler_params=pltpu.CompilerParams(
                collective_id=0, has_side_effects=True, vmem_limit_bytes=56 * 1024 * 1024
            ),
        )(tokens, hidden_cot, gate_pre, up_pre)

    in_specs = (
        P(("dp", "col"), "row"),
        P(("dp", "row"), "col"),
        P(("dp", "row"), "col"),
        P(("dp", "row"), "col"),
    )
    return jax.shard_map(
        on_device, mesh=mesh, in_specs=in_specs, out_specs=P("row", "dp", "col"), check_vma=False
    )
```

```python
import functools
import math

import jax
import jax.numpy as jnp
from jax import lax
from jax.experimental import pallas as pl
from jax.experimental.pallas import tpu as pltpu
from jax.sharding import PartitionSpec as P

MESH = pl.DeviceIdType.MESH


def near_square(n):
    nx = math.isqrt(n)
    while n % nx:
        nx -= 1
    return n // nx, nx


def kernel(dims, plan, tok, cot, gate, up, out, ins, grads, toks, tokt, part, got,
           gx, part2, own2, got2, in_sem, own_sem, ty_s, ty_r, tz_s, tz_r, gy_s, gy_r, gp_s, gp_r, x_s, x_r,
           tx_s, tx_r, gx_s, gx_r, gq_s, gq_r, p2_s, p2_r):
    ny, nx, nr, nz, wide, block, chunks, cols = dims
    lead, ahead, own_at, per, lite = plan
    dp, r, z = lax.axis_index("dp"), lax.axis_index("row"), lax.axis_index("col")
    y, x = dp // nx, dp % nx
    subs = wide // block
    away = (nx - 1) * subs
    blocks = nx * subs
    plain = chunks - lite
    every = blocks + (2 if lite else 0)
    last = every - 1
    rows = ny * nr * grads.shape[3]

    def at(oy=0, ox=0, orow=0, oz=0):
        return {
            "dp": (y + oy) % ny * nx + (x + ox) % nx,
            "row": (r + orow) % nr,
            "col": (z + oz) % nz,
        }

    def remote(src, dst, ss, rs, to):
        return pltpu.make_async_remote_copy(
            src_ref=src, dst_ref=dst, send_sem=ss, recv_sem=rs, device_id=to, device_id_type=MESH)

    def span(low, high, f):
        def body(i, c):
            f(i)
            return c
        lax.fori_loop(low, high, body, 0)

    def load(k, i):
        at_cols = pl.ds(0, cols) if k == 0 else pl.ds(cols, (chunks - 1) * cols)
        return pltpu.make_async_copy((cot, gate, up)[i].at[:, at_cols], ins.at[i, :, at_cols], in_sem.at[i, k])

    def loads(k, act):
        for i in range(3):
            act(load(k, i))

    def tok_cols(oy, b):
        o, sub = (b // subs + 1) % nx, b % subs
        first = ((y + oy) % ny * nx + (x + o) % nx) * wide + sub * block
        return tok.at[:, pl.ds(pl.multiple_of(first, block), block)]

    def tok_of(oy, ox, sub):
        first = ((y + oy) % ny * nx + (x + ox) % nx) * wide + sub * block
        return tok.at[:, pl.ds(pl.multiple_of(first, block), block)]

    def tok_x(i):
        dst = toks.at[blocks + i, x, z]
        return remote(tok_of(1 - i, 1, subs - 1), dst, tx_s.at[0], tx_r.at[i], at(ox=1))

    def own_more():
        return pltpu.make_async_copy(tok_of(1, 0, subs - 1), toks.at[blocks, x, z], own_sem.at[blocks])

    def source(b, oy):
        return (jnp.where(b >= blocks, x, y) - oy + ny) % ny

    def own_tok(b):
        return pltpu.make_async_copy(tok_cols(0, b), toks.at[b, y, z], own_sem.at[b])

    def tok_y(oy, b):
        return remote(tok_cols(oy, b), toks.at[b, y, z], ty_s.at[oy - 1], ty_r.at[oy - 1, b], at(oy=oy))

    reach = min(2, nz - 1)
    hops = ([(d, 0) for d in range(reach, 0, -1)] + [(1, d) for d in range(2, nz - 1)])
    relays = max(nz - 3, 0)

    def valid(way, far, back):
        left = z >= back if way > 0 else z + back < nz
        right = z + far < nz if way > 0 else z >= far
        return jnp.logical_and(left, right)

    def relay_sem(w, back, b, oy):
        w = w if nz > 4 else 0
        return every + ((w * relays + back - 2) * every + b) * ny + oy

    def goes_on(way, far, back):
        if not 2 <= far + back <= nz - 2:
            return jnp.bool_(False)
        beyond = z + way * (far + 1)
        return beyond < nz if way > 0 else beyond >= 0

    def tok_z(b, oy, way, i):
        far, back = hops[i]
        ref = toks.at[b, source(b, oy), z - way * back]
        w, dist = (0 if way > 0 else 1), far + back
        sem = jnp.where(goes_on(way, far, back), relay_sem(w, dist, b, oy), b)
        return remote(ref, ref, tz_s.at[w, jnp.where(b >= blocks + 1, 1, 0)], tz_r.at[sem], at(oz=way * far + nz))

    def each_hop(relay, act):
        for way in (1, -1):
            for i, (far, back) in sorted(enumerate(hops), key=lambda h: way * h[1][0]):
                if (back > 0) == relay:
                    pl.when(valid(way, far, back))(functools.partial(act, way, i))

    def send_z(b, oy, part):
        def go(way, i):
            far, back = hops[i]
            send = tok_z(b, oy, way, i).start
            if part == "far":
                pl.when(goes_on(way, far, back))(send)
            else:
                pl.when(jnp.logical_not(goes_on(way, far, back)))(send)
        each_hop(False, go)

    def relay_z(group, b):
        for oy in group:
            def go(way, i, oy=oy):
                back = hops[i][1]
                ref = toks.at[b, source(b, oy), z - way * back]
                w = 0 if way > 0 else 1
                remote(ref, ref, tz_s.at[w, 0], tz_r.at[relay_sem(w, back, b, oy)], at(oz=1)).wait_recv()
                tok_z(b, oy, way, i).start()
            each_hop(True, go)

    def all_z(b, slots=ny):
        count = nz - 1
        for way in (1, -1):
            for far, back in hops:
                if back:
                    count = count - valid(way, far, back).astype(jnp.int32)
        for n in range(1, nz):
            ref = toks.at[b, pl.ds(0, slots), pl.ds(0, n)]
            pl.when(count == n)(remote(ref, ref, tz_s.at[0, 0], tz_r.at[b], at(oz=1)).wait_recv)

    def sent_z():
        for way in (1, -1):
            w = 0 if way > 0 else 1
            count = jnp.int32(0)
            for far, back in hops:
                count = count + valid(way, far, back).astype(jnp.int32)
            for n in range(1, nz):
                most = blocks + 1 if lite else blocks
                ref = toks.at[pl.ds(0, most), :, pl.ds(0, n)]
                pl.when(count == n)(remote(ref, ref, tz_s.at[w, 0], tz_r.at[0], at(oz=1)).wait_send)
                if lite:
                    ref = toks.at[last, pl.ds(0, 1), pl.ds(0, n)]
                    pl.when(count == n)(remote(ref, ref, tz_s.at[w, 1], tz_r.at[0], at(oz=1)).wait_send)

    def grad_y(oy, k):
        ref = grads.at[k, y, r]
        return remote(ref, ref, gy_s.at[oy - 1], gy_r.at[oy - 1, k], at(oy=oy))

    def grad_p(orow, oy, k):
        ref = grads.at[k, (y - oy + ny) % ny, r]
        return remote(ref, ref, gp_s.at[orow - 1], gp_r.at[orow - 1, k], at(orow=orow))

    def got_p(orow, k):
        ref = grads.at[k, :, (r - orow + nr) % nr]
        remote(ref, ref, gp_s.at[orow - 1], gp_r.at[orow - 1, k], at(orow=orow)).wait_recv()

    def sum_x(b, k):
        at_rows = pl.ds(pl.multiple_of(b * block, block), block)
        sent = x_s.at[jnp.where(k >= plain, 1, 0)]
        return remote(part.at[k, at_rows], got.at[k, at_rows], sent, x_r.at[k], at(ox=b // subs + 1))

    def grad_x(i):
        return remote(grads.at[plain + i, y, r], gx.at[i, x, r], gx_s.at[0], gx_r.at[i], at(ox=1))

    def grad_q(i, ox):
        dst = gx.at[i, (x + ox) % nx, r]
        src = dst if ox else grads.at[plain + i, y, r]
        return remote(src, dst, gq_s.at[0], gq_r.at[i], at(orow=1))

    def got_q(i):
        ref = gx.at[i, :, (r + 1) % nr]
        remote(ref, ref, gq_s.at[0], gq_r.at[i], at(orow=1)).wait_recv()

    def sum_y(i):
        return remote(part2.at[i], got2.at[i], p2_s.at[0], p2_r.at[i], at(oy=1))

    span(0, blocks, lambda b: own_tok(b).start())
    if lite:
        own_more().start()

    for k in range(2):
        loads(k, lambda c: c.start())

    peers = ([at(oy=o) for o in range(1, ny)] + [at(ox=o) for o in range(1, nx)]
             + [at(orow=o) for o in range(1, nr)])
    barrier = pltpu.get_barrier_semaphore()

    def greet(to):
        pl.semaphore_signal(barrier, inc=1, device_id=to, device_id_type=MESH)
    for to in peers:
        greet(to)
    met = jnp.int32(len(peers))
    for far in range(1, reach + 1):
        for way in (1, -1):
            there = valid(way, far, 0)
            pl.when(there)(functools.partial(greet, at(oz=way * far + nz)))
            met = met + there.astype(jnp.int32)
    pl.semaphore_wait(barrier, met)

    def tok_out(b):
        for oy in range(1, ny):
            tok_y(oy, b).start()

    def own_out(b):
        pl.when(b < blocks)(lambda: own_tok(b).wait())
        if lite:
            pl.when(b == blocks)(lambda: own_more().wait())
        send_z(b, 0, "far")

    def pass_on(b):
        for oy in range(1, ny):
            pl.when(b < blocks)(lambda: tok_y(oy, b).wait_recv())
            if lite:
                pl.when(b >= blocks)(lambda: tok_x(b - blocks).wait_recv())
            send_z(b, oy, "far")
            send_z(b, oy, "rest")

    def gate_grad(k):
        for g in range(2):
            pl.when(k == g)(functools.partial(loads, g, lambda c: c.wait()))
        step = 32
        tall = ins.shape[1]
        at_cols = pl.ds(pl.multiple_of(k * cols, cols), cols)

        def rows_of(j, c):
            at_rows = pl.ds(pl.multiple_of(j * step, step), step)
            h = ins[0, at_rows, at_cols].astype(jnp.float32)
            g = ins[1, at_rows, at_cols].astype(jnp.float32)
            u = ins[2, at_rows, at_cols].astype(jnp.float32)
            s = jax.nn.sigmoid(g)
            grads[k, y, r, at_rows, :] = (h * u * s * (1.0 + g * (1.0 - s))).astype(grads.dtype)
            return c
        lax.fori_loop(0, tall // step, rows_of, 0)
        for orow in range(1, nr):
            grad_p(orow, 0, k).start()

    def feed(k):
        pl.when(k < plain)(lambda: gate_grad(k))
        for oy in range(1, ny):
            grad_y(oy, k).start()
        pl.when(k + 1 < blocks)(lambda: tok_out(k + 1))

    def take_block(b):
        all_z(b)
        first = pl.multiple_of(b * block, block)
        tokt[pl.ds(first, block), :] = toks[b].reshape(rows, block).T

    def tile(b, k):
        at_rows = pl.ds(pl.multiple_of(b * block, block), block)
        right = grads[k].reshape(rows, cols)
        sums = jnp.dot(tokt[at_rows, :], right, preferred_element_type=jnp.float32)
        part[k, at_rows, :] = sums.astype(part.dtype)
        sum_x(b, k).start()

    def finish(k):
        left = tokt[away * block:blocks * block, :]
        sums = jnp.dot(left, grads[k].reshape(rows, cols), preferred_element_type=jnp.float32)
        remote(got.at[k], got.at[k], x_s.at[0], x_r.at[k], at(ox=1)).wait_recv()
        for o in range(nx - 1):
            sums = sums + got[k, o * wide:(o + 1) * wide, :].astype(jnp.float32)
        out[0, :, pl.ds(pl.multiple_of(k * cols, cols), cols)] = sums.astype(out.dtype)

    def catch_up(k, b):
        take_block(b)
        span(0, k, functools.partial(tile, b))

    def pass_step(j):
        pass_on(j)
        pl.when(j + 1 < blocks)(lambda: own_out(j + 1))

    passed = lambda k: jnp.minimum(jnp.minimum(k + 2, blocks) + more(k, chunks - 5) + more(k, chunks - 4), every)
    own_blocks = blocks + 1 if lite else blocks

    def rest(b):
        if lite:
            pl.when(b == blocks)(lambda: own_out(b))
        pl.when(b < own_blocks)(lambda: send_z(b, 0, "rest"))

    own_relay = functools.partial(relay_z, (0,))
    got_relay = functools.partial(relay_z, range(1, ny))
    more = lambda k, at_step: jnp.where(k >= at_step, 1, 0)
    early = lambda k: jnp.minimum(jnp.minimum(relayed(k) + 1, blocks) + more(k, chunks - 3), own_blocks)
    relayed = lambda k: jnp.minimum(
        jnp.clip(jnp.where(k < away, k + 1, away + (k - away) * 5 // 6), 0, blocks)
        + more(k, chunks - 3) + more(k, chunks - 2), every)
    ready = lambda k: jnp.clip(k, 1, away)
    ended = lambda k: jnp.clip((k - own_at + 1) * per, 0, jnp.minimum(jnp.clip(k - 1, 0, plain), 2 * per))

    tok_out(0)
    own_out(0)
    rest(0)
    if lite:
        for i in range(2):
            tok_x(i).start()
    span(0, lead, feed)

    def over_x(i):
        gate_grad(plain + i)
        grad_x(i).start()
        grad_q(i, 0).start()
    if lite:
        over_x(0)
    pass_step(0)
    if lite:
        span(1, lite, over_x)
    span(lead, ahead, feed)
    own_relay(0)

    def over_y():
        for i in range(lite):
            grad_x(i).wait_recv()
            grad_q(i, 1).start()
        take_block(blocks)
        all_z(last, 1)
        toks[last, x] = toks[blocks - 1, y]
        tokt[last * block:, :] = toks[last].reshape(rows, block).T

        def sums(i):
            got_q(i)
            gx[i, x, r] = grads[plain + i, y, r]
            both = jnp.dot(tokt[blocks * block:, :], gx[i].reshape(rows, cols), preferred_element_type=jnp.float32)
            part2[i] = both[:block].astype(part2.dtype)
            sum_y(i).start()
            own2[i] = both[block:]
        span(0, lite, sums)

    def finish_last(i):
        k, most = plain + i, (away - 1) * block
        total = jnp.dot(tokt[away * block:away * block + most, :], grads[k].reshape(rows, cols),
                        preferred_element_type=jnp.float32)
        at_rows = pl.ds(0, most)
        remote(got.at[k, at_rows], got.at[k, at_rows], x_s.at[1], x_r.at[k], at(ox=1)).wait_recv()
        at_cols = pl.ds(pl.multiple_of(k * cols, cols), cols)
        out[0, 0:most, at_cols] = (total + got[k, 0:most, :].astype(jnp.float32)).astype(out.dtype)
        sum_y(i).wait_recv()
        out[0, most:, at_cols] = (own2[i] + got2[i].astype(jnp.float32)).astype(out.dtype)

    def main(k, c):
        late = k == away
        span(jnp.where(late, away, ready(k - 1)), ready(k), functools.partial(catch_up, k))
        for oy in range(1, ny):
            grad_y(oy, k).wait_recv()
            for orow in range(1, nr):
                grad_p(orow, oy, k).start()
        before = jnp.where(k > 0, relayed(k - 1), 0)
        span(before, relayed(k), got_relay)
        span(jnp.where(late, ready(k - 1), away), away, functools.partial(catch_up, k))
        span(passed(k - 1), passed(k), rest)
        span(early(k - 1), early(k), own_relay)
        span(passed(k - 1), passed(k), pass_step)
        pl.when(k + ahead < chunks)(lambda: feed(k + ahead))
        pl.when(k == 0)(lambda: take_block(0))
        for orow in range(1, nr):
            got_p(orow, k)
        span(0, jnp.where(k >= plain, away - 1, ready(k)), lambda b: tile(b, k))

        @pl.when(k == own_at)
        def _():
            span(away, blocks, take_block)
        if lite:
            pl.when(k == chunks - 2)(over_y)
        span(ended(k - 1), ended(k), finish)
        return c
    lax.fori_loop(0, chunks, main, 0)
    span(ended(chunks - 1), plain, finish)
    if lite:
        span(0, lite, finish_last)

    for oy in range(1, ny):
        ref = toks.at[pl.ds(0, blocks), y, z]
        remote(ref, ref, ty_s.at[oy - 1], ty_r.at[oy - 1, 0], at(oy=oy)).wait_send()
        ref = grads.at[:, y, r]
        remote(ref, ref, gy_s.at[oy - 1], gy_r.at[oy - 1, 0], at(oy=oy)).wait_send()
    for orow in range(1, nr):
        ref = grads.at[:, :, r]
        remote(ref, ref, gp_s.at[orow - 1], gp_r.at[orow - 1, 0], at(orow=orow)).wait_send()
    sent_z()
    ref = part.at[pl.ds(0, plain)]
    remote(ref, ref, x_s.at[0], x_r.at[0], at(ox=1)).wait_send()
    if lite:
        ref = part.at[pl.ds(plain, lite), pl.ds(0, (away - 1) * block)]
        remote(ref, ref, x_s.at[1], x_r.at[0], at(ox=1)).wait_send()
        ref = toks.at[pl.ds(blocks, 2), x, z]
        remote(ref, ref, tx_s.at[0], tx_r.at[0], at(ox=1)).wait_send()
        ref = grads.at[pl.ds(plain, lite), y, r]
        remote(ref, ref, gx_s.at[0], gx_r.at[0], at(ox=1)).wait_send()
        ref = gx.at[:, :, r]
        remote(ref, ref, gq_s.at[0], gq_r.at[0], at(orow=1)).wait_send()
        remote(part2, part2, p2_s.at[0], p2_r.at[0], at(oy=1)).wait_send()


def solution(mesh):
    ndp, nr, nz = mesh.shape["dp"], mesh.shape["row"], mesh.shape["col"]
    ny, nx = near_square(ndp)

    def on_device(tokens, hidden_cot, gate_pre, up_pre):
        tok_rows, wid = tokens.shape
        tall, hidden = gate_pre.shape
        wide = wid // ndp
        block = math.gcd(wide, 128)
        cols = math.gcd(hidden, 256)
        chunks = hidden // cols
        subs = wide // block
        blocks, away = nx * subs, (nx - 1) * subs
        rows = ny * nz * tok_rows
        lite = 3 if nx == ny == nr == 2 and subs > 1 and chunks > 10 else 0
        every = blocks + (2 if lite else 0)
        more = max(lite, 1)
        relays = (2 if nz > 4 else 1) * max(nz - 3, 0) * every * ny
        dims = (ny, nx, nr, nz, wide, block, chunks, cols)
        plan = (3, min(5, chunks), max(chunks - 4, 0), 3, lite)
        dma = pltpu.SemaphoreType.DMA
        dt = tokens.dtype
        return pl.pallas_call(
            functools.partial(kernel, dims, plan),
            out_shape=pltpu.VMEM((1, wide, hidden), dt),
            in_specs=[pl.BlockSpec(memory_space=pl.ANY)] * 4,
            out_specs=pl.BlockSpec(memory_space=pltpu.VMEM),
            scratch_shapes=[
                pltpu.VMEM((3, tall, hidden), dt),
                pltpu.VMEM((chunks, ny, nr, tall, cols), dt),
                pltpu.VMEM((every, ny, nz, tok_rows, block), dt),
                pltpu.VMEM((every * block, rows), dt),
                pltpu.VMEM((chunks, away * block, cols), dt),
                pltpu.VMEM((chunks, away * block, cols), dt),
                pltpu.VMEM((more, nx, nr, tall, cols), dt) if lite else pltpu.VMEM((1, 1, 1, 16, 128), dt),
                pltpu.VMEM((more, block, cols), dt),
                pltpu.VMEM((more, block, cols), jnp.float32),
                pltpu.VMEM((more, block, cols), dt),
                dma((3, 2)),
                dma((every,)),
                dma((ny - 1,)),
                dma((ny - 1, blocks)),
                dma((2, 2)),
                dma((every + relays,)),
                dma((ny - 1,)),
                dma((ny - 1, chunks)),
                dma((nr - 1,)),
                dma((nr - 1, chunks)),
                dma((2,)),
                dma((chunks,)),
                dma((1,)),
                dma((2,)),
                dma((1,)),
                dma((more,)),
                dma((1,)),
                dma((more,)),
                dma((1,)),
                dma((more,)),
            ],
            compiler_params=pltpu.CompilerParams(
                collective_id=0, has_side_effects=True, vmem_limit_bytes=56 * 1024 * 1024
            ),
        )(tokens, hidden_cot, gate_pre, up_pre)

    in_specs = (
        P(("dp", "col"), "row"),
        P(("dp", "row"), "col"),
        P(("dp", "row"), "col"),
        P(("dp", "row"), "col"),
    )
    return jax.shard_map(
        on_device, mesh=mesh, in_specs=in_specs, out_specs=P("row", "dp", "col"), check_vma=False
    )
```

```python
import functools
import math

import jax
import jax.numpy as jnp
from jax import lax
from jax.experimental import pallas as pl
from jax.experimental.pallas import tpu as pltpu
from jax.sharding import PartitionSpec as P

MESH = pl.DeviceIdType.MESH


def near_square(n):
    nx = math.isqrt(n)
    while n % nx:
        nx -= 1
    return n // nx, nx


def kernel(dims, plan, tok, cot, gate, up, out, ins, grads, toks, tokt, part, got,
           gx, part2, own2, got2, in_sem, own_sem, ty_s, ty_r, tz_s, tz_r, gy_s, gy_r, gp_s, gp_r, x_s, x_r,
           tx_s, tx_r, gx_s, gx_r, gq_s, gq_r, p2_s, p2_r, two_in):
    ny, nx, nr, nz, wide, block, chunks, cols = dims
    lead, ahead, own_at, per, lite = plan
    dp, r, z = lax.axis_index("dp"), lax.axis_index("row"), lax.axis_index("col")
    y, x = dp // nx, dp % nx
    subs = wide // block
    away = (nx - 1) * subs
    blocks = nx * subs
    plain = chunks - lite
    every = blocks + (2 if lite else 0)
    last = every - 1
    rows = ny * nr * grads.shape[3]

    def at(oy=0, ox=0, orow=0, oz=0):
        return {
            "dp": (y + oy) % ny * nx + (x + ox) % nx,
            "row": (r + orow) % nr,
            "col": (z + oz) % nz,
        }

    def remote(src, dst, ss, rs, to):
        return pltpu.make_async_remote_copy(
            src_ref=src, dst_ref=dst, send_sem=ss, recv_sem=rs, device_id=to, device_id_type=MESH)

    def span(low, high, f):
        def body(i, c):
            f(i)
            return c
        lax.fori_loop(low, high, body, 0)

    def load(k, i):
        at_cols = pl.ds(0, cols) if k == 0 else pl.ds(cols, (chunks - 1) * cols)
        return pltpu.make_async_copy((cot, gate, up)[i].at[:, at_cols], ins.at[i, :, at_cols], in_sem.at[i, k])

    def loads(k, act):
        for i in range(3):
            act(load(k, i))

    def tok_cols(oy, b):
        o, sub = (b // subs + 1) % nx, b % subs
        first = ((y + oy) % ny * nx + (x + o) % nx) * wide + sub * block
        return tok.at[:, pl.ds(pl.multiple_of(first, block), block)]

    def tok_of(oy, ox, sub):
        first = ((y + oy) % ny * nx + (x + ox) % nx) * wide + sub * block
        return tok.at[:, pl.ds(pl.multiple_of(first, block), block)]

    def tok_x(i):
        dst = toks.at[blocks + i, x, z]
        return remote(tok_of(1 - i, 1, subs - 1), dst, tx_s.at[0], tx_r.at[i], at(ox=1))

    def own_more():
        return pltpu.make_async_copy(tok_of(1, 0, subs - 1), toks.at[blocks, x, z], own_sem.at[blocks])

    def source(b, oy):
        return (jnp.where(b >= blocks, x, y) - oy + ny) % ny

    def own_tok(b):
        return pltpu.make_async_copy(tok_cols(0, b), toks.at[b, y, z], own_sem.at[b])

    def tok_y(oy, b):
        return remote(tok_cols(oy, b), toks.at[b, y, z], ty_s.at[oy - 1], ty_r.at[oy - 1, b], at(oy=oy))

    reach = min(2, nz - 1)
    hops = ([(d, 0) for d in range(reach, 0, -1)] + [(1, d) for d in range(2, nz - 1)])
    relays = max(nz - 3, 0)

    def inside(way, far):
        return z + far < nz if way > 0 else z >= far

    def valid(way, far, back):
        return jnp.logical_and(inside(-way, back), inside(way, far))

    def relay_sem(w, back, b, oy):
        w = w if nz > 4 else 0
        return every + ((w * relays + back - 2) * every + b) * ny + oy

    def goes_on(way, far, back):
        if not 2 <= far + back <= nz - 2:
            return jnp.bool_(False)
        beyond = z + way * (far + 1)
        return beyond < nz if way > 0 else beyond >= 0

    def tok_z(b, oy, way, i):
        far, back = hops[i]
        ref = toks.at[b, source(b, oy), z - way * back]
        w, dist = (0 if way > 0 else 1), far + back
        sem = jnp.where(goes_on(way, far, back), relay_sem(w, dist, b, oy), b)
        return remote(ref, ref, tz_s.at[w, jnp.where(b >= blocks + 1, 1, 0)], tz_r.at[sem], at(oz=way * far + nz))

    def each_hop(relay, act):
        for way in (1, -1):
            for i, (far, back) in sorted(enumerate(hops), key=lambda h: way * h[1][0]):
                if (back > 0) == relay:
                    pl.when(valid(way, far, back))(functools.partial(act, way, i))

    def send_z(b, oy, part):
        def go(way, i):
            far, back = hops[i]
            send = tok_z(b, oy, way, i).start
            if part in ("one", "two"):
                if far == (1 if part == "one" else 2):
                    send()
            elif part == "far":
                pl.when(goes_on(way, far, back))(send)
            else:
                pl.when(jnp.logical_not(goes_on(way, far, back)))(send)
        each_hop(False, go)

    def relay_z(group, b):
        for oy in group:
            def go(way, i, oy=oy):
                back = hops[i][1]
                ref = toks.at[b, source(b, oy), z - way * back]
                w = 0 if way > 0 else 1
                remote(ref, ref, tz_s.at[w, 0], tz_r.at[relay_sem(w, back, b, oy)], at(oz=1)).wait_recv()
                tok_z(b, oy, way, i).start()
            each_hop(True, go)

    def all_z(b, slots=ny):
        count = nz - 1
        for way in (1, -1):
            for far, back in hops:
                if back:
                    count = count - valid(way, far, back).astype(jnp.int32)
        for n in range(1, nz):
            ref = toks.at[b, pl.ds(0, slots), pl.ds(0, n)]
            pl.when(count == n)(remote(ref, ref, tz_s.at[0, 0], tz_r.at[b], at(oz=1)).wait_recv)

    def sent_z():
        for way in (1, -1):
            w = 0 if way > 0 else 1
            count = jnp.int32(0)
            for far, back in hops:
                count = count + valid(way, far, back).astype(jnp.int32)
            for n in range(1, nz):
                most = blocks + 1 if lite else blocks
                ref = toks.at[pl.ds(0, most), :, pl.ds(0, n)]
                pl.when(count == n)(remote(ref, ref, tz_s.at[w, 0], tz_r.at[0], at(oz=1)).wait_send)
                if lite:
                    ref = toks.at[last, pl.ds(0, 1), pl.ds(0, n)]
                    pl.when(count == n)(remote(ref, ref, tz_s.at[w, 1], tz_r.at[0], at(oz=1)).wait_send)

    def grad_y(oy, k):
        ref = grads.at[k, y, r]
        return remote(ref, ref, gy_s.at[oy - 1], gy_r.at[oy - 1, k], at(oy=oy))

    def grad_p(orow, oy, k):
        ref = grads.at[k, (y - oy + ny) % ny, r]
        return remote(ref, ref, gp_s.at[orow - 1], gp_r.at[orow - 1, k], at(orow=orow))

    def got_p(orow, k):
        ref = grads.at[k, :, (r - orow + nr) % nr]
        remote(ref, ref, gp_s.at[orow - 1], gp_r.at[orow - 1, k], at(orow=orow)).wait_recv()

    def sum_x(b, k):
        at_rows = pl.ds(pl.multiple_of(b * block, block), block)
        sent = x_s.at[jnp.where(k >= plain, 1, 0)]
        return remote(part.at[k, at_rows], got.at[k, at_rows], sent, x_r.at[k], at(ox=b // subs + 1))

    def grad_x(i):
        return remote(grads.at[plain + i, y, r], gx.at[i, x, r], gx_s.at[0], gx_r.at[i], at(ox=1))

    def grad_q(i, ox):
        dst = gx.at[i, (x + ox) % nx, r]
        src = dst if ox else grads.at[plain + i, y, r]
        return remote(src, dst, gq_s.at[0], gq_r.at[i], at(orow=1))

    def got_q(i):
        ref = gx.at[i, :, (r + 1) % nr]
        remote(ref, ref, gq_s.at[0], gq_r.at[i], at(orow=1)).wait_recv()

    def sum_y(i):
        return remote(part2.at[i], got2.at[i], p2_s.at[0], p2_r.at[i], at(oy=1))

    span(0, blocks, lambda b: own_tok(b).start())
    if lite:
        own_more().start()

    for k in range(2):
        loads(k, lambda c: c.start())

    peers = ([at(oy=o) for o in range(1, ny)] + [at(ox=o) for o in range(1, nx)]
             + [at(orow=o) for o in range(1, nr)])
    barrier = pltpu.get_barrier_semaphore()

    def greet(to):
        pl.semaphore_signal(barrier, inc=1, device_id=to, device_id_type=MESH)
    for to in peers:
        greet(to)
    met = jnp.int32(len(peers))
    for way in (1, -1):
        there = inside(way, 1)
        pl.when(there)(functools.partial(greet, at(oz=way + nz)))
        met = met + jnp.where(there, 1, 0)
    pl.semaphore_wait(barrier, met)

    def say_on(way):
        pl.semaphore_signal(two_in.at[max(way, 0)], inc=1, device_id=at(oz=way + nz), device_id_type=MESH)
    for way in (1, -1):
        pl.when(jnp.logical_and(inside(-way, 1), inside(way, 1)))(functools.partial(say_on, way))

    def meet():
        for way in (1, -1):
            pl.when(inside(-way, 2))(lambda w=max(way, 0): pl.semaphore_wait(two_in.at[w], 1))

    def tok_out(b):
        for oy in range(1, ny):
            tok_y(oy, b).start()

    def own_out(b):
        pl.when(b < blocks)(lambda: own_tok(b).wait())
        if lite:
            pl.when(b == blocks)(lambda: own_more().wait())
        send_z(b, 0, "far")

    def pass_on(b):
        for oy in range(1, ny):
            pl.when(b < blocks)(lambda: tok_y(oy, b).wait_recv())
            if lite:
                pl.when(b >= blocks)(lambda: tok_x(b - blocks).wait_recv())
            send_z(b, oy, "far")
            send_z(b, oy, "rest")

    def gate_grad(k):
        for g in range(2):
            pl.when(k == g)(functools.partial(loads, g, lambda c: c.wait()))
        step = 32
        tall = ins.shape[1]
        at_cols = pl.ds(pl.multiple_of(k * cols, cols), cols)

        def rows_of(j, c):
            at_rows = pl.ds(pl.multiple_of(j * step, step), step)
            h = ins[0, at_rows, at_cols].astype(jnp.float32)
            g = ins[1, at_rows, at_cols].astype(jnp.float32)
            u = ins[2, at_rows, at_cols].astype(jnp.float32)
            s = jax.nn.sigmoid(g)
            grads[k, y, r, at_rows, :] = (h * u * s * (1.0 + g * (1.0 - s))).astype(grads.dtype)
            return c
        lax.fori_loop(0, tall // step, rows_of, 0)
        for orow in range(1, nr):
            grad_p(orow, 0, k).start()

    def feed(k):
        pl.when(k < plain)(lambda: gate_grad(k))
        for oy in range(1, ny):
            grad_y(oy, k).start()
        pl.when(k + 1 < blocks)(lambda: tok_out(k + 1))

    def take_block(b):
        all_z(b)
        first = pl.multiple_of(b * block, block)
        tokt[pl.ds(first, block), :] = toks[b].reshape(rows, block).T

    def tile(b, k):
        at_rows = pl.ds(pl.multiple_of(b * block, block), block)
        right = grads[k].reshape(rows, cols)
        sums = jnp.dot(tokt[at_rows, :], right, preferred_element_type=jnp.float32)
        part[k, at_rows, :] = sums.astype(part.dtype)
        sum_x(b, k).start()

    def finish(k):
        left = tokt[away * block:blocks * block, :]
        sums = jnp.dot(left, grads[k].reshape(rows, cols), preferred_element_type=jnp.float32)
        remote(got.at[k], got.at[k], x_s.at[0], x_r.at[k], at(ox=1)).wait_recv()
        for o in range(nx - 1):
            sums = sums + got[k, o * wide:(o + 1) * wide, :].astype(jnp.float32)
        out[0, :, pl.ds(pl.multiple_of(k * cols, cols), cols)] = sums.astype(out.dtype)

    def catch_up(k, b):
        take_block(b)
        span(0, k, functools.partial(tile, b))

    def pass_step(j):
        pass_on(j)
        pl.when(j + 1 < blocks)(lambda: own_out(j + 1))

    passed = lambda k: jnp.minimum(jnp.minimum(k + 2, blocks) + more(k, chunks - 5) + more(k, chunks - 4), every)
    own_blocks = blocks + 1 if lite else blocks

    def rest(b):
        if lite:
            pl.when(b == blocks)(lambda: own_out(b))
        pl.when(b < own_blocks)(lambda: send_z(b, 0, "rest"))

    own_relay = functools.partial(relay_z, (0,))
    got_relay = functools.partial(relay_z, range(1, ny))
    more = lambda k, at_step: jnp.where(k >= at_step, 1, 0)
    early = lambda k: jnp.minimum(jnp.minimum(relayed(k) + 1, blocks) + more(k, chunks - 3), own_blocks)
    relayed = lambda k: jnp.minimum(
        jnp.clip(jnp.where(k < away, k + 1, away + (k - away) * 5 // 6), 0, blocks)
        + more(k, chunks - 3) + more(k, chunks - 2), every)
    ready = lambda k: jnp.clip(k, 1, away)
    ended = lambda k: jnp.clip((k - own_at + 1) * per, 0, jnp.minimum(jnp.clip(k - 1, 0, plain), 2 * per))

    tok_out(0)
    own_tok(0).wait()
    send_z(0, 0, "one")
    if lite:
        for i in range(2):
            tok_x(i).start()
    span(0, 1, feed)
    meet()
    send_z(0, 0, "two")
    span(1, lead, feed)

    def over_x(i):
        gate_grad(plain + i)
        grad_x(i).start()
        grad_q(i, 0).start()
    if lite:
        over_x(0)
    pass_step(0)
    if lite:
        span(1, lite, over_x)
    span(lead, ahead, feed)
    own_relay(0)

    def over_y():
        for i in range(lite):
            grad_x(i).wait_recv()
            grad_q(i, 1).start()
        take_block(blocks)
        all_z(last, 1)
        toks[last, x] = toks[blocks - 1, y]
        tokt[last * block:, :] = toks[last].reshape(rows, block).T

        def sums(i):
            got_q(i)
            gx[i, x, r] = grads[plain + i, y, r]
            both = jnp.dot(tokt[blocks * block:, :], gx[i].reshape(rows, cols), preferred_element_type=jnp.float32)
            part2[i] = both[:block].astype(part2.dtype)
            sum_y(i).start()
            own2[i] = both[block:]
        span(0, lite, sums)

    def finish_last(i):
        k, most = plain + i, (away - 1) * block
        total = jnp.dot(tokt[away * block:away * block + most, :], grads[k].reshape(rows, cols),
                        preferred_element_type=jnp.float32)
        at_rows = pl.ds(0, most)
        remote(got.at[k, at_rows], got.at[k, at_rows], x_s.at[1], x_r.at[k], at(ox=1)).wait_recv()
        at_cols = pl.ds(pl.multiple_of(k * cols, cols), cols)
        out[0, 0:most, at_cols] = (total + got[k, 0:most, :].astype(jnp.float32)).astype(out.dtype)
        sum_y(i).wait_recv()
        out[0, most:, at_cols] = (own2[i] + got2[i].astype(jnp.float32)).astype(out.dtype)

    def main(k, c):
        late = k == away
        span(jnp.where(late, away, ready(k - 1)), ready(k), functools.partial(catch_up, k))
        for oy in range(1, ny):
            grad_y(oy, k).wait_recv()
            for orow in range(1, nr):
                grad_p(orow, oy, k).start()
        before = jnp.where(k > 0, relayed(k - 1), 0)
        span(before, relayed(k), got_relay)
        span(jnp.where(late, ready(k - 1), away), away, functools.partial(catch_up, k))
        span(passed(k - 1), passed(k), rest)
        span(early(k - 1), early(k), own_relay)
        span(passed(k - 1), passed(k), pass_step)
        pl.when(k + ahead < chunks)(lambda: feed(k + ahead))
        pl.when(k == 0)(lambda: take_block(0))
        for orow in range(1, nr):
            got_p(orow, k)
        span(0, jnp.where(k >= plain, away - 1, ready(k)), lambda b: tile(b, k))

        @pl.when(k == own_at)
        def _():
            span(away, blocks, take_block)
        if lite:
            pl.when(k == chunks - 2)(over_y)
        span(ended(k - 1), ended(k), finish)
        return c
    lax.fori_loop(0, chunks, main, 0)
    span(ended(chunks - 1), plain, finish)
    if lite:
        span(0, lite, finish_last)

    for oy in range(1, ny):
        ref = toks.at[pl.ds(0, blocks), y, z]
        remote(ref, ref, ty_s.at[oy - 1], ty_r.at[oy - 1, 0], at(oy=oy)).wait_send()
        ref = grads.at[:, y, r]
        remote(ref, ref, gy_s.at[oy - 1], gy_r.at[oy - 1, 0], at(oy=oy)).wait_send()
    for orow in range(1, nr):
        ref = grads.at[:, :, r]
        remote(ref, ref, gp_s.at[orow - 1], gp_r.at[orow - 1, 0], at(orow=orow)).wait_send()
    sent_z()
    ref = part.at[pl.ds(0, plain)]
    remote(ref, ref, x_s.at[0], x_r.at[0], at(ox=1)).wait_send()
    if lite:
        ref = part.at[pl.ds(plain, lite), pl.ds(0, (away - 1) * block)]
        remote(ref, ref, x_s.at[1], x_r.at[0], at(ox=1)).wait_send()
        ref = toks.at[pl.ds(blocks, 2), x, z]
        remote(ref, ref, tx_s.at[0], tx_r.at[0], at(ox=1)).wait_send()
        ref = grads.at[pl.ds(plain, lite), y, r]
        remote(ref, ref, gx_s.at[0], gx_r.at[0], at(ox=1)).wait_send()
        ref = gx.at[:, :, r]
        remote(ref, ref, gq_s.at[0], gq_r.at[0], at(orow=1)).wait_send()
        remote(part2, part2, p2_s.at[0], p2_r.at[0], at(oy=1)).wait_send()


def solution(mesh):
    ndp, nr, nz = mesh.shape["dp"], mesh.shape["row"], mesh.shape["col"]
    ny, nx = near_square(ndp)

    def on_device(tokens, hidden_cot, gate_pre, up_pre):
        tok_rows, wid = tokens.shape
        tall, hidden = gate_pre.shape
        wide = wid // ndp
        block = math.gcd(wide, 128)
        cols = math.gcd(hidden, 256)
        chunks = hidden // cols
        subs = wide // block
        blocks, away = nx * subs, (nx - 1) * subs
        rows = ny * nz * tok_rows
        lite = 3 if nx == ny == nr == 2 and subs > 1 and chunks > 10 else 0
        every = blocks + (2 if lite else 0)
        more = max(lite, 1)
        relays = (2 if nz > 4 else 1) * max(nz - 3, 0) * every * ny
        dims = (ny, nx, nr, nz, wide, block, chunks, cols)
        plan = (3, min(5, chunks), max(chunks - 4, 0), 3, lite)
        dma = pltpu.SemaphoreType.DMA
        dt = tokens.dtype
        return pl.pallas_call(
            functools.partial(kernel, dims, plan),
            out_shape=pltpu.VMEM((1, wide, hidden), dt),
            in_specs=[pl.BlockSpec(memory_space=pl.ANY)] * 4,
            out_specs=pl.BlockSpec(memory_space=pltpu.VMEM),
            scratch_shapes=[
                pltpu.VMEM((3, tall, hidden), dt),
                pltpu.VMEM((chunks, ny, nr, tall, cols), dt),
                pltpu.VMEM((every, ny, nz, tok_rows, block), dt),
                pltpu.VMEM((every * block, rows), dt),
                pltpu.VMEM((chunks, away * block, cols), dt),
                pltpu.VMEM((chunks, away * block, cols), dt),
                pltpu.VMEM((more, nx, nr, tall, cols), dt) if lite else pltpu.VMEM((1, 1, 1, 16, 128), dt),
                pltpu.VMEM((more, block, cols), dt),
                pltpu.VMEM((more, block, cols), jnp.float32),
                pltpu.VMEM((more, block, cols), dt),
                dma((3, 2)),
                dma((every,)),
                dma((ny - 1,)),
                dma((ny - 1, blocks)),
                dma((2, 2)),
                dma((every + relays,)),
                dma((ny - 1,)),
                dma((ny - 1, chunks)),
                dma((nr - 1,)),
                dma((nr - 1, chunks)),
                dma((2,)),
                dma((chunks,)),
                dma((1,)),
                dma((2,)),
                dma((1,)),
                dma((more,)),
                dma((1,)),
                dma((more,)),
                dma((1,)),
                dma((more,)),
                pltpu.SemaphoreType.REGULAR((2,)),
            ],
            compiler_params=pltpu.CompilerParams(
                collective_id=0, has_side_effects=True, vmem_limit_bytes=56 * 1024 * 1024
            ),
        )(tokens, hidden_cot, gate_pre, up_pre)

    in_specs = (
        P(("dp", "col"), "row"),
        P(("dp", "row"), "col"),
        P(("dp", "row"), "col"),
        P(("dp", "row"), "col"),
    )
    return jax.shard_map(
        on_device, mesh=mesh, in_specs=in_specs, out_specs=P("row", "dp", "col"), check_vma=False
    )
```

```python
import functools
import math

import jax
import jax.numpy as jnp
from jax import lax
from jax.experimental import pallas as pl
from jax.experimental.pallas import tpu as pltpu
from jax.sharding import PartitionSpec as P

MESH = pl.DeviceIdType.MESH


def near_square(n):
    nx = math.isqrt(n)
    while n % nx:
        nx -= 1
    return n // nx, nx


def kernel(dims, plan, tok, cot, gate, up, out, ins, grads, toks, tokt, part, got,
           gx, part2, own2, got2, in_sem, own_sem, ty_s, ty_r, tz_s, tz_r, gy_s, gy_r, gp_s, gp_r, x_s, x_r,
           tx_s, tx_r, gx_s, gx_r, gq_s, gq_r, p2_s, p2_r, two_in):
    ny, nx, nr, nz, wide, block, chunks, cols = dims
    lead, ahead, own_at, per, lite = plan
    dp, r, z = lax.axis_index("dp"), lax.axis_index("row"), lax.axis_index("col")
    y, x = dp // nx, dp % nx
    subs = wide // block
    away = (nx - 1) * subs
    blocks = nx * subs
    plain = chunks - lite
    every = blocks + (2 if lite else 0)
    last = every - 1
    rows = ny * nr * grads.shape[3]

    def at(oy=0, ox=0, orow=0, oz=0):
        return {
            "dp": (y + oy) % ny * nx + (x + ox) % nx,
            "row": (r + orow) % nr,
            "col": (z + oz) % nz,
        }

    def remote(src, dst, ss, rs, to):
        return pltpu.make_async_remote_copy(
            src_ref=src, dst_ref=dst, send_sem=ss, recv_sem=rs, device_id=to, device_id_type=MESH)

    def span(low, high, f):
        def body(i, c):
            f(i)
            return c
        lax.fori_loop(low, high, body, 0)

    def load(k, i):
        at_cols = pl.ds(0, cols) if k == 0 else pl.ds(cols, (chunks - 1) * cols)
        return pltpu.make_async_copy((cot, gate, up)[i].at[:, at_cols], ins.at[i, :, at_cols], in_sem.at[i, k])

    def loads(k, act):
        for i in range(3):
            act(load(k, i))

    def tok_cols(oy, b):
        o, sub = (b // subs + 1) % nx, b % subs
        first = ((y + oy) % ny * nx + (x + o) % nx) * wide + sub * block
        return tok.at[:, pl.ds(pl.multiple_of(first, block), block)]

    def tok_of(oy, ox, sub):
        first = ((y + oy) % ny * nx + (x + ox) % nx) * wide + sub * block
        return tok.at[:, pl.ds(pl.multiple_of(first, block), block)]

    def tok_x(i):
        dst = toks.at[blocks + i, x, z]
        return remote(tok_of(1 - i, 1, subs - 1), dst, tx_s.at[0], tx_r.at[i], at(ox=1))

    def own_more():
        return pltpu.make_async_copy(tok_of(1, 0, subs - 1), toks.at[blocks, x, z], own_sem.at[blocks])

    def source(b, oy):
        return (jnp.where(b >= blocks, x, y) - oy + ny) % ny

    def own_tok(b):
        return pltpu.make_async_copy(tok_cols(0, b), toks.at[b, y, z], own_sem.at[b])

    def tok_y(oy, b):
        return remote(tok_cols(oy, b), toks.at[b, y, z], ty_s.at[oy - 1], ty_r.at[oy - 1, b], at(oy=oy))

    reach = min(2, nz - 1)
    hops = ([(d, 0) for d in range(reach, 0, -1)] + [(1, d) for d in range(2, nz - 1)])
    relays = max(nz - 3, 0)

    def inside(way, far):
        return z + far < nz if way > 0 else z >= far

    def valid(way, far, back):
        return jnp.logical_and(inside(-way, back), inside(way, far))

    def relay_sem(w, back, b, oy):
        w = w if nz > 4 else 0
        return every + ((w * relays + back - 2) * every + b) * ny + oy

    def goes_on(way, far, back):
        if not 2 <= far + back <= nz - 2:
            return jnp.bool_(False)
        beyond = z + way * (far + 1)
        return beyond < nz if way > 0 else beyond >= 0

    def tok_z(b, oy, way, i):
        far, back = hops[i]
        ref = toks.at[b, source(b, oy), z - way * back]
        w, dist = (0 if way > 0 else 1), far + back
        sem = jnp.where(goes_on(way, far, back), relay_sem(w, dist, b, oy), b)
        return remote(ref, ref, tz_s.at[w, jnp.where(b >= blocks + 1, 1, 0)], tz_r.at[sem], at(oz=way * far + nz))

    def each_hop(relay, act):
        for way in (1, -1):
            for i, (far, back) in sorted(enumerate(hops), key=lambda h: way * h[1][0]):
                if (back > 0) == relay:
                    pl.when(valid(way, far, back))(functools.partial(act, way, i))

    def send_z(b, oy, part):
        def go(way, i):
            far, back = hops[i]
            send = tok_z(b, oy, way, i).start
            if part in ("one", "two"):
                if far == (1 if part == "one" else 2):
                    send()
            elif part == "far":
                pl.when(goes_on(way, far, back))(send)
            else:
                pl.when(jnp.logical_not(goes_on(way, far, back)))(send)
        each_hop(False, go)

    def relay_z(group, b):
        for oy in group:
            def go(way, i, oy=oy):
                back = hops[i][1]
                ref = toks.at[b, source(b, oy), z - way * back]
                w = 0 if way > 0 else 1
                remote(ref, ref, tz_s.at[w, 0], tz_r.at[relay_sem(w, back, b, oy)], at(oz=1)).wait_recv()
                tok_z(b, oy, way, i).start()
            each_hop(True, go)

    def all_z(b, slots=ny):
        count = nz - 1
        for way in (1, -1):
            for far, back in hops:
                if back:
                    count = count - valid(way, far, back).astype(jnp.int32)
        for n in range(1, nz):
            ref = toks.at[b, pl.ds(0, slots), pl.ds(0, n)]
            pl.when(count == n)(remote(ref, ref, tz_s.at[0, 0], tz_r.at[b], at(oz=1)).wait_recv)

    def sent_z():
        for way in (1, -1):
            w = 0 if way > 0 else 1
            count = jnp.int32(0)
            for far, back in hops:
                count = count + valid(way, far, back).astype(jnp.int32)
            for n in range(1, nz):
                most = blocks + 1 if lite else blocks
                ref = toks.at[pl.ds(0, most), :, pl.ds(0, n)]
                pl.when(count == n)(remote(ref, ref, tz_s.at[w, 0], tz_r.at[0], at(oz=1)).wait_send)
                if lite:
                    ref = toks.at[last, pl.ds(0, 1), pl.ds(0, n)]
                    pl.when(count == n)(remote(ref, ref, tz_s.at[w, 1], tz_r.at[0], at(oz=1)).wait_send)

    def grad_y(oy, k):
        ref = grads.at[k, y, r]
        return remote(ref, ref, gy_s.at[oy - 1], gy_r.at[oy - 1, k], at(oy=oy))

    def grad_p(orow, oy, k):
        ref = grads.at[k, (y - oy + ny) % ny, r]
        return remote(ref, ref, gp_s.at[orow - 1], gp_r.at[orow - 1, k], at(orow=orow))

    def got_p(orow, k):
        ref = grads.at[k, :, (r - orow + nr) % nr]
        remote(ref, ref, gp_s.at[orow - 1], gp_r.at[orow - 1, k], at(orow=orow)).wait_recv()

    def sum_x(b, k):
        at_rows = pl.ds(pl.multiple_of(b * block, block), block)
        sent = x_s.at[jnp.where(k >= plain, 1, 0)]
        return remote(part.at[k, at_rows], got.at[k, at_rows], sent, x_r.at[k], at(ox=b // subs + 1))

    def grad_x(i):
        return remote(grads.at[plain + i, y, r], gx.at[i, x, r], gx_s.at[0], gx_r.at[0], at(ox=1))

    def grad_q(i, ox):
        dst = gx.at[i, (x + ox) % nx, r]
        src = dst if ox else grads.at[plain + i, y, r]
        return remote(src, dst, gq_s.at[0], gq_r.at[0], at(orow=1))

    def got_q():
        ref = gx.at[:, :, (r + 1) % nr]
        remote(ref, ref, gq_s.at[0], gq_r.at[0], at(orow=1)).wait_recv()

    def sum_y(i):
        return remote(part2.at[i], got2.at[i], p2_s.at[0], p2_r.at[i], at(oy=1))

    span(0, blocks, lambda b: own_tok(b).start())
    if lite:
        own_more().start()

    for k in range(2):
        loads(k, lambda c: c.start())

    peers = ([at(oy=o) for o in range(1, ny)] + [at(ox=o) for o in range(1, nx)]
             + [at(orow=o) for o in range(1, nr)])
    barrier = pltpu.get_barrier_semaphore()

    def greet(to):
        pl.semaphore_signal(barrier, inc=1, device_id=to, device_id_type=MESH)
    for to in peers:
        greet(to)
    met = jnp.int32(len(peers))
    for way in (1, -1):
        there = inside(way, 1)
        pl.when(there)(functools.partial(greet, at(oz=way + nz)))
        met = met + jnp.where(there, 1, 0)
    pl.semaphore_wait(barrier, met)

    def say_on(way):
        pl.semaphore_signal(two_in.at[max(way, 0)], inc=1, device_id=at(oz=way + nz), device_id_type=MESH)
    for way in (1, -1):
        pl.when(jnp.logical_and(inside(-way, 1), inside(way, 1)))(functools.partial(say_on, way))

    def meet():
        for way in (1, -1):
            pl.when(inside(-way, 2))(lambda w=max(way, 0): pl.semaphore_wait(two_in.at[w], 1))

    def tok_out(b):
        for oy in range(1, ny):
            tok_y(oy, b).start()

    def own_out(b):
        pl.when(b < blocks)(lambda: own_tok(b).wait())
        if lite:
            pl.when(b == blocks)(lambda: own_more().wait())
        send_z(b, 0, "far")

    def pass_on(b):
        for oy in range(1, ny):
            pl.when(b < blocks)(lambda: tok_y(oy, b).wait_recv())
            if lite:
                pl.when(b >= blocks)(lambda: tok_x(b - blocks).wait_recv())
            send_z(b, oy, "far")
            send_z(b, oy, "rest")

    def gate_grad(k):
        for g in range(2):
            pl.when(k == g)(functools.partial(loads, g, lambda c: c.wait()))
        step = 32
        tall = ins.shape[1]
        at_cols = pl.ds(pl.multiple_of(k * cols, cols), cols)

        def rows_of(j, c):
            at_rows = pl.ds(pl.multiple_of(j * step, step), step)
            h = ins[0, at_rows, at_cols].astype(jnp.float32)
            g = ins[1, at_rows, at_cols].astype(jnp.float32)
            u = ins[2, at_rows, at_cols].astype(jnp.float32)
            s = jax.nn.sigmoid(g)
            grads[k, y, r, at_rows, :] = (h * u * s * (1.0 + g * (1.0 - s))).astype(grads.dtype)
            return c
        lax.fori_loop(0, tall // step, rows_of, 0)
        for orow in range(1, nr):
            grad_p(orow, 0, k).start()

    def feed(k):
        pl.when(k < plain)(lambda: gate_grad(k))
        for oy in range(1, ny):
            grad_y(oy, k).start()
        pl.when(k + 1 < blocks)(lambda: tok_out(k + 1))

    def take_block(b):
        all_z(b)
        first = pl.multiple_of(b * block, block)
        tokt[pl.ds(first, block), :] = toks[b].reshape(rows, block).T

    def tile(b, k):
        at_rows = pl.ds(pl.multiple_of(b * block, block), block)
        right = grads[k].reshape(rows, cols)
        sums = jnp.dot(tokt[at_rows, :], right, preferred_element_type=jnp.float32)
        part[k, at_rows, :] = sums.astype(part.dtype)
        sum_x(b, k).start()

    def finish(k):
        left = tokt[away * block:blocks * block, :]
        sums = jnp.dot(left, grads[k].reshape(rows, cols), preferred_element_type=jnp.float32)
        remote(got.at[k], got.at[k], x_s.at[0], x_r.at[k], at(ox=1)).wait_recv()
        for o in range(nx - 1):
            sums = sums + got[k, o * wide:(o + 1) * wide, :].astype(jnp.float32)
        out[0, :, pl.ds(pl.multiple_of(k * cols, cols), cols)] = sums.astype(out.dtype)

    def catch_up(k, b):
        take_block(b)
        span(0, k, functools.partial(tile, b))

    def pass_step(j):
        pass_on(j)
        pl.when(j + 1 < blocks)(lambda: own_out(j + 1))

    passed = lambda k: jnp.minimum(jnp.minimum(k + 2, blocks) + more(k, chunks - 5) + more(k, chunks - 4), every)
    own_blocks = blocks + 1 if lite else blocks

    def rest(b):
        if lite:
            pl.when(b == blocks)(lambda: own_out(b))
        pl.when(b < own_blocks)(lambda: send_z(b, 0, "rest"))

    own_relay = functools.partial(relay_z, (0,))
    got_relay = functools.partial(relay_z, range(1, ny))
    more = lambda k, at_step: jnp.where(k >= at_step, 1, 0)
    early = lambda k: jnp.minimum(jnp.minimum(relayed(k) + 1, blocks) + more(k, chunks - 3), own_blocks)
    relayed = lambda k: jnp.minimum(
        jnp.clip(jnp.where(k < away, k + 1, away + (k - away) * 5 // 6), 0, blocks)
        + more(k, chunks - 3) + more(k, chunks - 2), every)
    ready = lambda k: jnp.clip(k, 1, away)
    ended = lambda k: jnp.clip((k - own_at + 1) * per, 0, jnp.minimum(jnp.clip(k - 1, 0, plain), 2 * per))

    tok_out(0)
    own_tok(0).wait()
    send_z(0, 0, "one")
    if lite:
        for i in range(2):
            tok_x(i).start()
    span(0, 1, feed)
    meet()
    send_z(0, 0, "two")
    span(1, lead, feed)

    def over_x(i):
        gate_grad(plain + i)
        grad_x(i).start()
        grad_q(i, 0).start()
    if lite:
        over_x(0)
    pass_step(0)
    if lite:
        span(1, lite, over_x)
    span(lead, ahead, feed)
    own_relay(0)

    def over_y():
        ref = gx.at[:, (x + 1) % nx, r]
        remote(ref, ref, gx_s.at[0], gx_r.at[0], at(ox=1)).wait_recv()
        for i in range(lite):
            grad_q(i, 1).start()
        take_block(blocks)
        all_z(last, 1)
        toks[last, x] = toks[blocks - 1, y]
        tokt[last * block:, :] = toks[last].reshape(rows, block).T

        got_q()

        def sums(i):
            gx[i, x, r] = grads[plain + i, y, r]
            both = jnp.dot(tokt[blocks * block:, :], gx[i].reshape(rows, cols), preferred_element_type=jnp.float32)
            part2[i] = both[:block].astype(part2.dtype)
            sum_y(i).start()
            own2[i] = both[block:]
        span(0, lite, sums)

    def finish_last(i):
        k, most = plain + i, (away - 1) * block
        total = jnp.dot(tokt[away * block:away * block + most, :], grads[k].reshape(rows, cols),
                        preferred_element_type=jnp.float32)
        at_rows = pl.ds(0, most)
        remote(got.at[k, at_rows], got.at[k, at_rows], x_s.at[1], x_r.at[k], at(ox=1)).wait_recv()
        at_cols = pl.ds(pl.multiple_of(k * cols, cols), cols)
        out[0, 0:most, at_cols] = (total + got[k, 0:most, :].astype(jnp.float32)).astype(out.dtype)
        sum_y(i).wait_recv()
        out[0, most:, at_cols] = (own2[i] + got2[i].astype(jnp.float32)).astype(out.dtype)

    def main(k, c):
        late = k == away
        span(jnp.where(late, away, ready(k - 1)), ready(k), functools.partial(catch_up, k))
        for oy in range(1, ny):
            grad_y(oy, k).wait_recv()
            for orow in range(1, nr):
                grad_p(orow, oy, k).start()
        before = jnp.where(k > 0, relayed(k - 1), 0)
        span(before, relayed(k), got_relay)
        span(jnp.where(late, ready(k - 1), away), away, functools.partial(catch_up, k))
        span(passed(k - 1), passed(k), rest)
        span(early(k - 1), early(k), own_relay)
        span(passed(k - 1), passed(k), pass_step)
        pl.when(k + ahead < chunks)(lambda: feed(k + ahead))
        pl.when(k == 0)(lambda: take_block(0))
        for orow in range(1, nr):
            got_p(orow, k)
        span(0, jnp.where(k >= plain, away - 1, ready(k)), lambda b: tile(b, k))

        @pl.when(k == own_at)
        def _():
            span(away, blocks, take_block)
        if lite:
            pl.when(k == chunks - 2)(over_y)
        span(ended(k - 1), ended(k), finish)
        return c
    lax.fori_loop(0, chunks, main, 0)
    span(ended(chunks - 1), plain, finish)
    if lite:
        span(0, lite, finish_last)

    for oy in range(1, ny):
        ref = toks.at[pl.ds(0, blocks), y, z]
        remote(ref, ref, ty_s.at[oy - 1], ty_r.at[oy - 1, 0], at(oy=oy)).wait_send()
        ref = grads.at[:, y, r]
        remote(ref, ref, gy_s.at[oy - 1], gy_r.at[oy - 1, 0], at(oy=oy)).wait_send()
    for orow in range(1, nr):
        ref = grads.at[:, :, r]
        remote(ref, ref, gp_s.at[orow - 1], gp_r.at[orow - 1, 0], at(orow=orow)).wait_send()
    sent_z()
    ref = part.at[pl.ds(0, plain)]
    remote(ref, ref, x_s.at[0], x_r.at[0], at(ox=1)).wait_send()
    if lite:
        ref = part.at[pl.ds(plain, lite), pl.ds(0, (away - 1) * block)]
        remote(ref, ref, x_s.at[1], x_r.at[0], at(ox=1)).wait_send()
        ref = toks.at[pl.ds(blocks, 2), x, z]
        remote(ref, ref, tx_s.at[0], tx_r.at[0], at(ox=1)).wait_send()
        ref = grads.at[pl.ds(plain, lite), y, r]
        remote(ref, ref, gx_s.at[0], gx_r.at[0], at(ox=1)).wait_send()
        ref = gx.at[:, :, r]
        remote(ref, ref, gq_s.at[0], gq_r.at[0], at(orow=1)).wait_send()
        remote(part2, part2, p2_s.at[0], p2_r.at[0], at(oy=1)).wait_send()


def solution(mesh):
    ndp, nr, nz = mesh.shape["dp"], mesh.shape["row"], mesh.shape["col"]
    ny, nx = near_square(ndp)

    def on_device(tokens, hidden_cot, gate_pre, up_pre):
        tok_rows, wid = tokens.shape
        tall, hidden = gate_pre.shape
        wide = wid // ndp
        block = math.gcd(wide, 128)
        cols = math.gcd(hidden, 256)
        chunks = hidden // cols
        subs = wide // block
        blocks, away = nx * subs, (nx - 1) * subs
        rows = ny * nz * tok_rows
        lite = 3 if nx == ny == nr == 2 and subs > 1 and chunks > 10 else 0
        every = blocks + (2 if lite else 0)
        more = max(lite, 1)
        relays = (2 if nz > 4 else 1) * max(nz - 3, 0) * every * ny
        dims = (ny, nx, nr, nz, wide, block, chunks, cols)
        plan = (2, min(5, chunks), max(chunks - 4, 0), 3, lite)
        dma = pltpu.SemaphoreType.DMA
        dt = tokens.dtype
        return pl.pallas_call(
            functools.partial(kernel, dims, plan),
            out_shape=pltpu.VMEM((1, wide, hidden), dt),
            in_specs=[pl.BlockSpec(memory_space=pl.ANY)] * 4,
            out_specs=pl.BlockSpec(memory_space=pltpu.VMEM),
            scratch_shapes=[
                pltpu.VMEM((3, tall, hidden), dt),
                pltpu.VMEM((chunks, ny, nr, tall, cols), dt),
                pltpu.VMEM((every, ny, nz, tok_rows, block), dt),
                pltpu.VMEM((every * block, rows), dt),
                pltpu.VMEM((chunks, away * block, cols), dt),
                pltpu.VMEM((chunks, away * block, cols), dt),
                pltpu.VMEM((more, nx, nr, tall, cols), dt) if lite else pltpu.VMEM((1, 1, 1, 16, 128), dt),
                pltpu.VMEM((more, block, cols), dt),
                pltpu.VMEM((more, block, cols), jnp.float32),
                pltpu.VMEM((more, block, cols), dt),
                dma((3, 2)),
                dma((every,)),
                dma((ny - 1,)),
                dma((ny - 1, blocks)),
                dma((2, 2)),
                dma((every + relays,)),
                dma((ny - 1,)),
                dma((ny - 1, chunks)),
                dma((nr - 1,)),
                dma((nr - 1, chunks)),
                dma((2,)),
                dma((chunks,)),
                dma((1,)),
                dma((2,)),
                dma((1,)),
                dma((1,)),
                dma((1,)),
                dma((1,)),
                dma((1,)),
                dma((more,)),
                pltpu.SemaphoreType.REGULAR((2,)),
            ],
            compiler_params=pltpu.CompilerParams(
                collective_id=0, has_side_effects=True, vmem_limit_bytes=56 * 1024 * 1024
            ),
        )(tokens, hidden_cot, gate_pre, up_pre)

    in_specs = (
        P(("dp", "col"), "row"),
        P(("dp", "row"), "col"),
        P(("dp", "row"), "col"),
        P(("dp", "row"), "col"),
    )
    return jax.shard_map(
        on_device, mesh=mesh, in_specs=in_specs, out_specs=P("row", "dp", "col"), check_vma=False
    )
```
